32 devices in a mesh: dom: 32 (over z, y, x, core).
Axes of the slice: x: 2, y: 2, z: 4, core: 2. Of those that a mesh axis runs over, the one named last changes fastest.
Arguments:
- field: float32 [3, 180224], P(None, 'dom'), may hold values from -6 to 6
- blocks: bfloat16 [30, 30, 131072], P(None, None, 'dom'), may hold values from -1 to 1
- connectivity: int32 [10, 131072], P(None, 'dom'), may hold values from 0 to 8703, as said below
- send_nodes: int32 [8, 12288], P(None, 'dom'), may hold values from 0 to 5631
- live_blocks: int32 [32], replicated, may hold values from 1 to 8
Outputs:
- image: float32 [3, 180224], P(None, 'dom')
The draws below stay inside these ranges and needn't reach their ends.
Inputs may be any that keep to these rules, and one draw needn't show every extreme that they name: `connectivity`: entries below 5632 name nodes of the element's own subdomain; entry 5632 + k * 384 + g names the node sent as entry g of row k by subdomain d - o_k, and only where that subdomain exists. `send_nodes`: columns d * 384 to (d + 1) * 384 - 1 of row k list local indices of nodes that subdomain d owns, in the order in which subdomain d + o_k numbers its ghost slots from d. Subdomain d's elements fill its first 512 * live_blocks[d] slots; the other slots are unused.
All inputs are finite; a program needn't handle non-finite values.
Results may differ from the reference program's by a relative error of at most 0.0003.
Values sent between devices are 32-bit elements; how exact they have to be, the bound alone decides.
A program may use at most 64 MiB of HBM per device.

```python
import jax
import jax.numpy as jnp
from jax import lax

ELEM_DEV = 4096
BLK = 512
REACH = 4
NODE_DEV = 5632
GHOST = 384
NBLK = 8
NODES = 180224
ELEMS = 131072
N_DOM = 32


def draw_connectivity(key, part):
    slot_total = N_DOM * ELEM_DEV
    key_local, key_ghost, key_pick = jax.random.split(jax.random.fold_in(key, 11), 3)
    local_ids = jax.random.randint(key_local, (10, slot_total), 0, NODE_DEV)
    ghost_ids = jax.random.randint(key_ghost, (10, slot_total), 0, 2 * REACH * GHOST)
    picked = jax.random.randint(key_pick, (10, slot_total), 0, 5) == 0
    device = jnp.arange(slot_total, dtype=jnp.int32)[None, :] // ELEM_DEV
    bucket = ghost_ids // GHOST
    offset = jnp.where(bucket < REACH, bucket + 1, REACH - 1 - bucket)
    source = device - offset
    usable = picked & (source >= 0) & (source < N_DOM)
    return jnp.where(usable, NODE_DEV + ghost_ids, local_ids).astype(jnp.int32)


def plant(values, key, low, high):
    spot = [jax.random.randint(jax.random.fold_in(key, axis), (), 0, length) for axis, length in enumerate(values.shape)]
    longest = values.shape.index(max(values.shape))
    beside = spot[:longest] + [(spot[longest] + 1) % values.shape[longest]] + spot[longest + 1:]
    return values.at[tuple(spot)].set(low).at[tuple(beside)].set(high)


def block_scale(stream_key, shape, cuts, smallest, high):
    factor_of, own = 1.0, jax.random.fold_in(stream_key, 6)
    for position, shards_of in cuts:
        steps = jnp.exp(jax.random.uniform(jax.random.fold_in(own, position), (shards_of,), jnp.float32, smallest / len(cuts), high / len(cuts)))
        factor_of = factor_of * jnp.repeat(steps, shape[position] // shards_of).reshape([-1 if axis == position else 1 for axis in range(len(shape))])
    return factor_of


def noise(stream_key, dims, scale, most, shards=(), kind=jnp.bfloat16):
    gain = block_scale(stream_key, dims, shards, -0.22, 0.18) if shards else 1.0
    drawn = jax.random.normal(stream_key, dims, jnp.float32) * scale * gain
    return jnp.minimum(jnp.maximum(drawn, -most), most).astype(kind)


def setup_inputs(seed: int = 0) -> dict:
    arg_keys = jax.random.split(jax.random.key(seed), 6)
    field = noise(arg_keys[0], (3, NODES), 1.0, 6.0, ((1, 32),), jnp.float32)
    blocks = noise(arg_keys[1], (30, 30, ELEMS), 30 ** -0.5, 1.0, ((2, 32),))
    connectivity = draw_connectivity(jax.random.fold_in(arg_keys[5], 71), 0)
    send_nodes = plant(jax.random.randint(arg_keys[3], (2 * REACH, N_DOM * GHOST), 0, NODE_DEV), jax.random.fold_in(arg_keys[3], 1), 0, NODE_DEV - 1).astype(jnp.int32)
    live_blocks = plant(jax.random.randint(arg_keys[4], (N_DOM,), NBLK // 8, NBLK + 1), jax.random.fold_in(arg_keys[4], 1), NBLK // 8, NBLK).astype(jnp.int32)
    return {"field": field, "blocks": blocks, "connectivity": connectivity, "send_nodes": send_nodes, "live_blocks": live_blocks}


def reference(field, blocks, connectivity, send_nodes, live_blocks):
    node_total = N_DOM * NODE_DEV
    offsets = jnp.array([k + 1 if k < REACH else REACH - 1 - k for k in range(2 * REACH)], jnp.int32)
    padded = jnp.concatenate([field, jnp.zeros((3, 1), field.dtype)], axis=1)

    def partition_step(totals, device):
        local_ids = device * NODE_DEV + jnp.arange(NODE_DEV, dtype=jnp.int32)
        pieces = [local_ids]
        for k in range(2 * REACH):
            source = device - offsets[k]
            inside = (source >= 0) & (source < N_DOM)
            clipped = jnp.clip(source, 0, N_DOM - 1).astype(jnp.int32)
            sent_rows = lax.dynamic_slice_in_dim(send_nodes[k], clipped * GHOST, GHOST)
            pieces.append(jnp.where(inside, clipped * NODE_DEV + sent_rows, node_total).astype(jnp.int32))
        global_ids = jnp.concatenate(pieces)
        element_nodes = lax.dynamic_slice_in_dim(connectivity, (device * ELEM_DEV).astype(jnp.int32), ELEM_DEV, 1)
        node_ids = global_ids[element_nodes]
        values = padded[:, node_ids].reshape(30, ELEM_DEV)
        stiffness = lax.dynamic_slice_in_dim(blocks, (device * ELEM_DEV).astype(jnp.int32), ELEM_DEV, 2).astype(jnp.float32)
        forces = jnp.einsum("ije,je->ie", stiffness, values, precision=lax.Precision.HIGHEST)
        live_mask = jnp.arange(ELEM_DEV, dtype=jnp.int32) < live_blocks[device] * BLK
        forces = jnp.where(live_mask[None, :], forces, 0.0)
        totals = totals.at[:, node_ids.reshape(-1)].add(forces.reshape(3, 10 * ELEM_DEV))
        return totals, None

    totals = jnp.zeros((3, node_total + 1), jnp.float32)
    totals, _ = lax.scan(partition_step, totals, jnp.arange(N_DOM, dtype=jnp.int32))
    return totals[:, :node_total]
```

```python
import functools

import jax
import jax.numpy as jnp
from jax import lax
from jax.experimental import pallas as pl
from jax.experimental.pallas import tpu as pltpu
from jax.sharding import PartitionSpec as P

BLK = 512
LOW = 256
LANES = 128
MESH = pl.DeviceIdType.MESH
VM = pl.BlockSpec(memory_space=pltpu.VMEM)


def round_up(n, m):
    return -(-n // m) * m


def split_parts(x):
    high = x.astype(jnp.bfloat16)
    low = (x - high.astype(jnp.float32)).astype(jnp.bfloat16)
    return high, low


def lower_hot(indices):
    lower = jnp.bitwise_and(indices, LOW - 1)
    rows = lax.broadcasted_iota(jnp.int32, (LOW, indices.shape[1]), 0)
    return jnp.where(rows == lower, 1.0, 0.0).astype(jnp.bfloat16)


def upper_mask(indices, height):
    upper = jnp.right_shift(indices, LOW.bit_length() - 1)
    return lax.broadcasted_iota(jnp.int32, (height, indices.shape[1]), 0) == upper


def pick(parts, hot, mask, height):
    spread = jnp.dot(parts, hot, preferred_element_type=jnp.float32)
    rows = []
    for c in range(3):
        whole = spread[c * height:(c + 1) * height] + spread[(3 + c) * height:(4 + c) * height]
        rows.append(jnp.sum(jnp.where(mask, whole, 0.0), axis=0, keepdims=True))
    return rows


def spread_back(rows, hot, mask):
    pairs = [split_parts(row) for row in rows]
    stacked = [jnp.where(mask, pair[p].astype(jnp.float32), 0.0) for p in range(2) for pair in pairs]
    placed = jnp.concatenate(stacked, axis=0).astype(jnp.bfloat16)
    return lax.dot_general(
        placed, hot, (((1,), (1,)), ((), ())), preferred_element_type=jnp.float32
    )


def put_segments(table, height, first, source, c, width):
    for t in range(width // LANES):
        s = first + t
        row, col = c * height + s * LANES // LOW, s * LANES % LOW
        table[row:row + 1, col:col + LANES] = source(t)


def make_parts(table):
    high, low = split_parts(table[...])
    return jnp.concatenate([high, low], axis=0)


def pick_kernel(height, field_ref, send_ref, out_ref, table):
    nodes = field_ref.shape[1]
    table[...] = jnp.zeros_like(table)
    for c in range(3):
        put_segments(
            table, height, 0, lambda t: field_ref[c:c + 1, t * LANES:(t + 1) * LANES], c, nodes
        )
    parts = make_parts(table)
    for k in range(send_ref.shape[0]):
        indices = send_ref[k:k + 1, :]
        rows = pick(parts, lower_hot(indices), upper_mask(indices, height), height)
        for c in range(3):
            out_ref[k, c:c + 1, :] = rows[c]


def exchange_kernel(sign, devices, offsets, in_ref, out_ref, send_sem, recv_sem):
    me = lax.axis_index("dom")
    barrier = pltpu.get_barrier_semaphore()
    count = 0
    for o in offsets:
        other = me + o
        inside = (other >= 0) & (other < devices)
        count = count + inside.astype(jnp.int32)

        @pl.when(inside)
        def _():
            pl.semaphore_signal(barrier, inc=1, device_id=(other,), device_id_type=MESH)

    pl.semaphore_wait(barrier, count)

    def copy_of(k):
        return pltpu.make_async_remote_copy(
            src_ref=in_ref.at[k],
            dst_ref=out_ref.at[k],
            send_sem=send_sem.at[k],
            recv_sem=recv_sem.at[k],
            device_id=(me + sign * offsets[k],),
            device_id_type=MESH,
        )

    def inside_of(k, way):
        other = me + way * sign * offsets[k]
        return (other >= 0) & (other < devices)

    order = sorted(range(len(offsets)), key=lambda k: -abs(offsets[k]))
    for k in order:

        @pl.when(inside_of(k, 1))
        def _():
            copy_of(k).start()

    for k in order:

        @pl.when(jnp.logical_not(inside_of(k, -1)))
        def _():
            out_ref[k] = jnp.zeros(out_ref.shape[1:], jnp.float32)

    for k in order:

        @pl.when(inside_of(k, 1))
        def _():
            copy_of(k).wait_send()

        @pl.when(inside_of(k, -1))
        def _():
            copy_of(k).wait_recv()


def exchange(values, sign, devices, offsets):
    return pl.pallas_call(
        functools.partial(exchange_kernel, sign, devices, offsets),
        out_shape=jax.ShapeDtypeStruct(values.shape, jnp.float32),
        in_specs=[VM],
        out_specs=VM,
        scratch_shapes=[
            pltpu.SemaphoreType.DMA((len(offsets),)),
            pltpu.SemaphoreType.DMA((len(offsets),)),
        ],
        compiler_params=pltpu.CompilerParams(
            collective_id=0 if sign > 0 else 1, has_side_effects=True
        ),
        name="exchange_out" if sign > 0 else "exchange_back",
    )(values)


def element_kernel(
    height, live_ref, field_ref, ghost_ref, conn_ref, block_ref, owned_ref, back_ref,
    table, parts, total, values,
):
    step = pl.program_id(0)
    nodes = field_ref.shape[1]
    reach, _, bucket = ghost_ref.shape

    @pl.when(step == 0)
    def _():
        table[...] = jnp.zeros_like(table)
        total[...] = jnp.zeros_like(total)
        for c in range(3):
            put_segments(
                table, height, 0, lambda t: field_ref[c:c + 1, t * LANES:(t + 1) * LANES], c, nodes
            )
            for k in range(reach):
                put_segments(
                    table, height, (nodes + k * bucket) // LANES,
                    lambda t: ghost_ref[k, c:c + 1, t * LANES:(t + 1) * LANES], c, bucket,
                )
        parts[...] = make_parts(table)

    @pl.when(step < live_ref[lax.axis_index("dom")])
    def _():
        corners = conn_ref.shape[0]
        for a in range(corners):
            indices = conn_ref[a:a + 1, :]
            rows = pick(parts[...], lower_hot(indices), upper_mask(indices, height), height)
            for c in range(3):
                values[c * corners + a:c * corners + a + 1, :] = rows[c]
        v = values[...]
        forces = [
            jnp.sum(block_ref[i].astype(jnp.float32) * v, axis=0, keepdims=True)
            for i in range(3 * corners)
        ]
        for a in range(corners):
            indices = conn_ref[a:a + 1, :]
            total[...] += spread_back(
                [forces[c * corners + a] for c in range(3)],
                lower_hot(indices),
                upper_mask(indices, height),
            )

    @pl.when(step == pl.num_programs(0) - 1)
    def _():
        table[...] = total[:3 * height, :] + total[3 * height:, :]

        def segment(c, s):
            row, col = c * height + s * LANES // LOW, s * LANES % LOW
            return table[row:row + 1, col:col + LANES]

        for c in range(3):
            for t in range(nodes // LANES):
                owned_ref[c:c + 1, t * LANES:(t + 1) * LANES] = segment(c, t)
            for k in range(reach):
                for t in range(bucket // LANES):
                    back_ref[k, c:c + 1, t * LANES:(t + 1) * LANES] = segment(
                        c, (nodes + k * bucket) // LANES + t
                    )


def add_kernel(height, owned_ref, in_ref, send_ref, out_ref, total):
    nodes = owned_ref.shape[1]
    acc = jnp.zeros((6 * height, LOW), jnp.float32)
    for k in range(send_ref.shape[0]):
        indices = send_ref[k:k + 1, :]
        acc = acc + spread_back(
            [in_ref[k, c:c + 1, :] for c in range(3)],
            lower_hot(indices),
            upper_mask(indices, height),
        )
    total[...] = acc[:3 * height] + acc[3 * height:]
    for c in range(3):
        for t in range(nodes // LANES):
            row, col = c * height + t * LANES // LOW, t * LANES % LOW
            span = slice(t * LANES, (t + 1) * LANES)
            out_ref[c:c + 1, span] = owned_ref[c:c + 1, span] + total[row:row + 1, col:col + LANES]


def body(field, blocks, connectivity, send_nodes, live_blocks):
    devices = lax.axis_size("dom")
    nodes = field.shape[1]
    reach2, bucket = send_nodes.shape
    reach = reach2 // 2
    offsets = [k + 1 if k < reach else reach - 1 - k for k in range(reach2)]
    corners, elements = connectivity.shape
    dofs = 3 * corners
    own_height = round_up(-(-nodes // LOW), 8)
    full_height = round_up(-(-(nodes + reach2 * bucket) // LOW), 8)
    ghost_shape = jax.ShapeDtypeStruct((reach2, 3, bucket), jnp.float32)
    field_shape = jax.ShapeDtypeStruct((3, nodes), jnp.float32)

    outgoing = pl.pallas_call(
        functools.partial(pick_kernel, own_height),
        out_shape=ghost_shape,
        in_specs=[VM, VM],
        out_specs=VM,
        scratch_shapes=[pltpu.VMEM((3 * own_height, LOW), jnp.float32)],
        name="pick_sent",
    )(field, send_nodes)
    ghosts = exchange(outgoing, 1, devices, offsets)

    whole = lambda *shape: pl.BlockSpec(shape, lambda b, live: (0,) * len(shape))
    owned, back = pl.pallas_call(
        functools.partial(element_kernel, full_height),
        out_shape=(field_shape, ghost_shape),
        grid_spec=pltpu.PrefetchScalarGridSpec(
            num_scalar_prefetch=1,
            grid=(elements // BLK,),
            in_specs=[
                whole(3, nodes),
                whole(reach2, 3, bucket),
                pl.BlockSpec((corners, BLK), lambda b, live: (0, b)),
                pl.BlockSpec((dofs, dofs, BLK), lambda b, live: (0, 0, b)),
            ],
            out_specs=[whole(3, nodes), whole(reach2, 3, bucket)],
            scratch_shapes=[
                pltpu.VMEM((3 * full_height, LOW), jnp.float32),
                pltpu.VMEM((6 * full_height, LOW), jnp.bfloat16),
                pltpu.VMEM((6 * full_height, LOW), jnp.float32),
                pltpu.VMEM((dofs, BLK), jnp.float32),
            ],
        ),
        compiler_params=pltpu.CompilerParams(dimension_semantics=("arbitrary",)),
        name="elements",
    )(live_blocks, field, ghosts, connectivity, blocks)

    returned = exchange(back, -1, devices, offsets)
    return pl.pallas_call(
        functools.partial(add_kernel, own_height),
        out_shape=field_shape,
        in_specs=[VM, VM, VM],
        out_specs=VM,
        scratch_shapes=[pltpu.VMEM((3 * own_height, LOW), jnp.float32)],
        name="add_returned",
    )(owned, returned, send_nodes)


def solution(mesh):
    return jax.shard_map(
        body,
        mesh=mesh,
        in_specs=(P(None, "dom"), P(None, None, "dom"), P(None, "dom"), P(None, "dom"), P()),
        out_specs=P(None, "dom"),
        check_vma=False,
    )
```

```python
import functools

import jax
import jax.numpy as jnp
from jax import lax
from jax.experimental import pallas as pl
from jax.experimental.pallas import tpu as pltpu
from jax.sharding import PartitionSpec as P

BLK = 512
LOW = 256
LANES = 128
MESH = pl.DeviceIdType.MESH
VM = pl.BlockSpec(memory_space=pltpu.VMEM)


def round_up(n, m):
    return -(-n // m) * m


def split_parts(x):
    high = x.astype(jnp.bfloat16)
    low = (x - high.astype(jnp.float32)).astype(jnp.bfloat16)
    return high, low


def narrow(x):
    return x.astype(jnp.float32).astype(jnp.bfloat16)


def row_numbers(height, width):
    return narrow(lax.broadcasted_iota(jnp.int32, (height, width), 0))


def lower_hot(indices):
    lower = narrow(jnp.bitwise_and(indices, LOW - 1))
    one, zero = jnp.bfloat16(1), jnp.bfloat16(0)
    return jnp.where(row_numbers(LOW, indices.shape[1]) == lower, one, zero)


def upper_of(indices):
    return jnp.right_shift(indices, LOW.bit_length() - 1)


def pick(parts, indices, height):
    spread = jnp.dot(parts, lower_hot(indices), preferred_element_type=jnp.float32)
    spread = spread[:3 * height] + spread[3 * height:]
    upper = upper_of(indices)
    sub = lax.broadcasted_iota(jnp.int32, (8, indices.shape[1]), 0)
    masks = [sub == upper - u for u in range(0, height, 8)]
    rows = []
    for c in range(3):
        found = jnp.zeros(sub.shape, jnp.float32)
        for t, mask in enumerate(masks):
            at = c * height + 8 * t
            found = jnp.where(mask, spread[at:at + 8], found)
        rows.append(jnp.sum(found, axis=0, keepdims=True))
    return rows


def spread_back(rows, indices, height):
    hot = lower_hot(indices)
    mask = row_numbers(height, indices.shape[1]) == narrow(upper_of(indices))
    pairs = [split_parts(row) for row in rows]
    placed = jnp.concatenate(
        [jnp.where(mask, pair[p], jnp.bfloat16(0)) for p in range(2) for pair in pairs], axis=0
    )
    return lax.dot_general(
        placed, hot, (((1,), (1,)), ((), ())), preferred_element_type=jnp.float32
    )


def put_segments(table, height, first, source, c, width):
    for t in range(width // LANES):
        s = first + t
        row, col = c * height + s * LANES // LOW, s * LANES % LOW
        table[row:row + 1, col:col + LANES] = source(t)


def make_parts(table):
    high, low = split_parts(table[...])
    return jnp.concatenate([high, low], axis=0)


def load_field(table, height, field_ref):
    table[...] = jnp.zeros_like(table)
    for c in range(3):
        put_segments(
            table, height, 0,
            lambda t: field_ref[c:c + 1, t * LANES:(t + 1) * LANES], c, field_ref.shape[1],
        )


def pick_kernel(
    height, devices, offsets, field_ref, send_ref, out_ref,
    table, parts, outgoing, send_sem, recv_sem,
):
    def before():
        load_field(table, height, field_ref)
        parts[...] = make_parts(table)
        for k in range(send_ref.shape[0]):
            rows = pick(parts[...], send_ref[k:k + 1, :], height)
            for c in range(3):
                outgoing[k, c:c + 1, :] = rows[c]

    exchange_kernel(
        1, devices, offsets, outgoing, out_ref, send_sem, recv_sem, before
    )


def nothing():
    pass


def exchange_kernel(
    sign, devices, offsets, in_ref, out_ref, send_sem, recv_sem, before=nothing, between=nothing
):
    me = lax.axis_index("dom")
    barrier = pltpu.get_barrier_semaphore()
    count = 0
    for o in offsets:
        other = me + o
        inside = (other >= 0) & (other < devices)
        count = count + inside.astype(jnp.int32)

        @pl.when(inside)
        def _():
            pl.semaphore_signal(barrier, inc=1, device_id=(other,), device_id_type=MESH)

    before()
    pl.semaphore_wait(barrier, count)

    def copy_of(k):
        return pltpu.make_async_remote_copy(
            src_ref=in_ref.at[k],
            dst_ref=out_ref.at[k],
            send_sem=send_sem.at[k],
            recv_sem=recv_sem.at[k],
            device_id=(me + sign * offsets[k],),
            device_id_type=MESH,
        )

    def inside_of(k, way):
        other = me + way * sign * offsets[k]
        return (other >= 0) & (other < devices)

    order = sorted(range(len(offsets)), key=lambda k: -abs(offsets[k]))
    for k in order:

        @pl.when(inside_of(k, 1))
        def _():
            copy_of(k).start()

    for k in order:

        @pl.when(jnp.logical_not(inside_of(k, -1)))
        def _():
            out_ref[k] = jnp.zeros(out_ref.shape[1:], jnp.float32)

    between()
    for k in order:

        @pl.when(inside_of(k, 1))
        def _():
            copy_of(k).wait_send()

        @pl.when(inside_of(k, -1))
        def _():
            copy_of(k).wait_recv()


def exchange(values, sign, devices, offsets):
    return pl.pallas_call(
        functools.partial(exchange_kernel, sign, devices, offsets),
        out_shape=jax.ShapeDtypeStruct(values.shape, jnp.float32),
        in_specs=[VM],
        out_specs=VM,
        scratch_shapes=[
            pltpu.SemaphoreType.DMA((len(offsets),)),
            pltpu.SemaphoreType.DMA((len(offsets),)),
        ],
        compiler_params=pltpu.CompilerParams(
            collective_id=0 if sign > 0 else 1, has_side_effects=True
        ),
        name="exchange_out" if sign > 0 else "exchange_back",
    )(values)


def element_kernel(
    low_height, height, live_ref, field_ref, ghost_ref, conn_ref, block_ref, owned_ref, back_ref,
    table, parts, total, values,
):
    step = pl.program_id(0)
    nodes = owned_ref.shape[1]
    reach, _, bucket = ghost_ref.shape

    @pl.when(step == 0)
    def _():
        load_field(table, low_height, field_ref)
        total[...] = jnp.zeros_like(total)
        for c in range(3):
            for k in range(reach):
                put_segments(
                    table, low_height, (nodes + k * bucket) // LANES,
                    lambda t: ghost_ref[k, c:c + 1, t * LANES:(t + 1) * LANES], c, bucket,
                )
        parts[...] = make_parts(table)

    @pl.when(step < live_ref[lax.axis_index("dom")])
    def _():
        corners = conn_ref.shape[0]
        for a in range(corners):
            rows = pick(parts[...], conn_ref[a:a + 1, :], low_height)
            for c in range(3):
                at = c * corners + a
                values[at:at + 1, :] = rows[c]
        v = values[...]
        forces = [
            jnp.sum(block_ref[i].astype(jnp.float32) * v, axis=0, keepdims=True)
            for i in range(3 * corners)
        ]
        for a in range(corners):
            total[...] += spread_back(
                [forces[c * corners + a] for c in range(3)], conn_ref[a:a + 1, :], height
            )

    @pl.when(step == pl.num_programs(0) - 1)
    def _():
        total[:3 * height, :] = total[:3 * height, :] + total[3 * height:, :]

        def segment(c, s):
            row, col = c * height + s * LANES // LOW, s * LANES % LOW
            return total[row:row + 1, col:col + LANES]

        for c in range(3):
            for t in range(nodes // LANES):
                owned_ref[c:c + 1, t * LANES:(t + 1) * LANES] = segment(c, t)
            for k in range(reach):
                for t in range(bucket // LANES):
                    back_ref[k, c:c + 1, t * LANES:(t + 1) * LANES] = segment(
                        c, (nodes + k * bucket) // LANES + t
                    )


def add_kernel(height, owned_ref, in_ref, send_ref, out_ref, total):
    nodes = owned_ref.shape[1]
    acc = jnp.zeros((6 * height, LOW), jnp.float32)
    for k in range(send_ref.shape[0]):
        acc = acc + spread_back(
            [in_ref[k, c:c + 1, :] for c in range(3)], send_ref[k:k + 1, :], height
        )
    total[...] = acc[:3 * height] + acc[3 * height:]
    for c in range(3):
        for t in range(nodes // LANES):
            row, col = c * height + t * LANES // LOW, t * LANES % LOW
            span = slice(t * LANES, (t + 1) * LANES)
            out_ref[c:c + 1, span] = owned_ref[c:c + 1, span] + total[row:row + 1, col:col + LANES]


def body(field, blocks, connectivity, send_nodes, live_blocks):
    devices = lax.axis_size("dom")
    nodes = field.shape[1]
    reach2, bucket = send_nodes.shape
    reach = reach2 // 2
    offsets = [k + 1 if k < reach else reach - 1 - k for k in range(reach2)]
    corners, elements = connectivity.shape
    dofs = 3 * corners
    own_height = round_up(-(-nodes // LOW), 8)
    full_height = round_up(-(-(nodes + reach2 * bucket) // LOW), 8)
    own_placed = round_up(-(-nodes // LOW), 16)
    all_placed = round_up(-(-(nodes + reach2 * bucket) // LOW), 16)
    ghost_shape = jax.ShapeDtypeStruct((reach2, 3, bucket), jnp.float32)
    field_shape = jax.ShapeDtypeStruct((3, nodes), jnp.float32)

    ghosts = pl.pallas_call(
        functools.partial(pick_kernel, own_height, devices, offsets),
        out_shape=ghost_shape,
        in_specs=[VM, VM],
        out_specs=VM,
        scratch_shapes=[
            pltpu.VMEM((3 * own_height, LOW), jnp.float32),
            pltpu.VMEM((3 * own_height * 2, LOW), jnp.bfloat16),
            pltpu.VMEM((reach2, 3, bucket), jnp.float32),
            pltpu.SemaphoreType.DMA((reach2,)),
            pltpu.SemaphoreType.DMA((reach2,)),
        ],
        compiler_params=pltpu.CompilerParams(collective_id=0, has_side_effects=True),
        name="pick_and_exchange",
    )(field, send_nodes)

    whole = lambda *shape: pl.BlockSpec(shape, lambda b, live: (0,) * len(shape))
    owned, back = pl.pallas_call(
        functools.partial(element_kernel, full_height, all_placed),
        out_shape=(field_shape, ghost_shape),
        grid_spec=pltpu.PrefetchScalarGridSpec(
            num_scalar_prefetch=1,
            grid=(elements // BLK,),
            in_specs=[
                whole(3, nodes),
                whole(reach2, 3, bucket),
                pl.BlockSpec((corners, BLK), lambda b, live: (0, b)),
                pl.BlockSpec((dofs, dofs, BLK), lambda b, live: (0, 0, b)),
            ],
            out_specs=[whole(3, nodes), whole(reach2, 3, bucket)],
            scratch_shapes=[
                pltpu.VMEM((3 * full_height, LOW), jnp.float32),
                pltpu.VMEM((3 * full_height * 2, LOW), jnp.bfloat16),
                pltpu.VMEM((6 * all_placed, LOW), jnp.float32),
                pltpu.VMEM((dofs, BLK), jnp.float32),
            ],
        ),
        compiler_params=pltpu.CompilerParams(dimension_semantics=("arbitrary",)),
        name="elements",
    )(live_blocks, field, ghosts, connectivity, blocks)

    returned = exchange(back, -1, devices, offsets)
    return pl.pallas_call(
        functools.partial(add_kernel, own_placed),
        out_shape=field_shape,
        in_specs=[VM, VM, VM],
        out_specs=VM,
        scratch_shapes=[pltpu.VMEM((3 * own_placed, LOW), jnp.float32)],
        name="add_returned",
    )(owned, returned, send_nodes)


def solution(mesh):
    return jax.shard_map(
        body,
        mesh=mesh,
        in_specs=(P(None, "dom"), P(None, None, "dom"), P(None, "dom"), P(None, "dom"), P()),
        out_specs=P(None, "dom"),
        check_vma=False,
    )
```
